32 devices in a mesh: seq: 8 (over z, y), batch: 4 (over x, core).
Axes of the slice: x: 2, y: 2, z: 4, core: 2. Of those that a mesh axis runs over, the one named last changes fastest.
Arguments:
- conv_input: bfloat16 [4096, 8192], P(('batch', 'seq')), parts along dimension 0, may hold values from -6 to 6
- gate_input: bfloat16 [4096, 8192], P(('batch', 'seq')), parts along dimension 0, may hold values from -6 to 6
- conv_weight: bfloat16 [4, 8192], P(None, 'seq'), may hold values from -3 to 3
- conv_bias: bfloat16 [8192], P('seq'), may hold values from -3 to 3
- x_weight: bfloat16 [8192, 288], P('seq'), may hold values from -0.0625 to 0.0625
- dt_gain: float32 [256], replicated, may hold values from 0.5 to 1.5
- dt_weight: bfloat16 [256, 8192], P(None, 'seq'), may hold values from -0.375 to 0.375
- dt_bias: float32 [8192], P('seq'), may hold values from -6.9 to -2.3
- a_log: float32 [16, 8192], P(None, 'seq'), may hold values from 0 to 2.77
- skip: float32 [8192], P('seq'), may hold values from 0.5 to 1.5
Outputs:
- mixed: bfloat16 [4096, 8192], P(('batch', 'seq')), parts along dimension 0
The draws below stay inside these ranges and needn't reach their ends.
There are 4 independent parts, one for each index of `batch`. The reference program is written for one: setup_inputs(seed, part) draws one part's arguments, and reference() takes and returns one part's arrays. A program takes and returns all parts, laid end to end along the dimension named above; an argument that names none is the same for every part. Nothing has to cross between parts.
All inputs are finite; a program needn't handle non-finite values.
Results may differ from the reference program's by a relative error of at most 0.0085.
Values may be sent and summed in bfloat16 or wider, within the bound.
A program may use at most 128 MiB of HBM per device.

```python
import jax
import jax.numpy as jnp
from jax import lax

INNER = 8192
STATE = 16
DT_RANK = 256
CONV = 4
LENGTH = 1024
PROJ = 288


def block_scale(key, extent, pieces, low, top_value):
    def one(axis_at, blocks):
        steps = jax.random.uniform(jax.random.fold_in(jax.random.fold_in(key, 6), axis_at), (blocks,), jnp.float32, low / len(pieces), top_value / len(pieces))
        return jnp.repeat(jnp.exp(steps), extent[axis_at] // blocks).reshape((-1,) + (1,) * (len(extent) - axis_at - 1))

    loudness = one(*pieces[0])
    for cut in pieces[1:]:
        loudness = loudness * one(*cut)
    return loudness


def centred(stream_key, shape, scale, limit, shards=(), kind=jnp.bfloat16):
    drawn = scale * jax.random.normal(stream_key, shape, jnp.float32)
    if shards:
        drawn = drawn * block_scale(stream_key, shape, shards, -0.22, 0.18)
    return jnp.clip(drawn, -limit, limit).astype(kind)


def setup_inputs(seed: int = 0, part: int = 0) -> dict:
    key_list = jax.random.split(jax.random.key(seed), 11)
    part_splits = jax.random.split(jax.random.fold_in(key_list[10], part), 11)
    conv_input = centred(part_splits[0], (LENGTH, INNER), 1.0, 6.0, ((0, 8),))
    gate_input = centred(part_splits[1], (LENGTH, INNER), 1.0, 6.0, ((0, 8),))
    conv_weight = centred(key_list[2], (CONV, INNER), CONV ** -0.5, 3.0, ((1, 8),))
    conv_bias = centred(key_list[3], (INNER,), 0.5, 3.0, ((0, 8),))
    x_weight = centred(key_list[4], (INNER, PROJ), INNER ** -0.5, 0.0625, ((0, 8),))
    dt_gain = jnp.clip(1.0 + 0.1 * jax.random.normal(key_list[5], (DT_RANK,), jnp.float32), 0.5, 1.5)
    dt_weight = centred(key_list[6], (DT_RANK, INNER), DT_RANK ** -0.5, 0.375, ((1, 8),))
    dt_bias = jnp.clip(-6.9 + 4.6000001430511475 * jax.random.uniform(key_list[7], (INNER,), jnp.float32) ** block_scale(key_list[7], (INNER,), ((0, 8),), -0.2, 0.2), -6.9, -2.3)
    a_log = jnp.clip(2.77 * jax.random.uniform(key_list[8], (STATE, INNER), jnp.float32) ** block_scale(key_list[8], (STATE, INNER), ((1, 8),), -0.2, 0.2), 0.0, 2.77)
    skip = jnp.clip(1.0 + 0.1 * jax.random.normal(key_list[9], (INNER,), jnp.float32), 0.5, 1.5)
    return dict(conv_input=conv_input, gate_input=gate_input, conv_weight=conv_weight, conv_bias=conv_bias, x_weight=x_weight, dt_gain=dt_gain, dt_weight=dt_weight, dt_bias=dt_bias, a_log=a_log, skip=skip)


def convolve(inputs, weight, bias):
    rows = inputs.shape[0]
    width = weight.shape[0]
    padded = jnp.concatenate([jnp.zeros((width - 1, inputs.shape[1]), jnp.float32), inputs.astype(jnp.float32)], 0)
    total = bias.astype(jnp.float32)[None, :]
    for tap in range(width):
        total = total + weight[tap].astype(jnp.float32)[None, :] * padded[tap:tap + rows]
    return jax.nn.silu(total).astype(jnp.bfloat16)

def reference(conv_input, gate_input, conv_weight, conv_bias, x_weight, dt_gain, dt_weight, dt_bias, a_log, skip):
    xc = convolve(conv_input, conv_weight, conv_bias)
    proj = jnp.dot(xc, x_weight, preferred_element_type=jnp.float32)
    dt_low = proj[:, :DT_RANK]
    bmat = proj[:, DT_RANK:DT_RANK + STATE]
    cmat = proj[:, DT_RANK + STATE:]
    normed = (dt_low * lax.rsqrt(lax.optimization_barrier(jnp.mean(dt_low * dt_low, axis=1, keepdims=True)) + 1e-06) * dt_gain[None, :]).astype(jnp.bfloat16)
    step = jax.nn.softplus(jnp.dot(normed, dt_weight, preferred_element_type=jnp.float32) + dt_bias[None, :])
    rate = -jnp.exp(a_log)
    xfloat = xc.astype(jnp.float32)

    def advance(state, inputs):
        step_t, x_t, b_t, c_t = inputs
        state = jnp.exp(step_t[None, :] * rate) * state + b_t[:, None] * (step_t * x_t)[None, :]
        return (state, lax.optimization_barrier(jnp.sum(c_t[:, None] * state, axis=0)))
    _, outputs = lax.scan(advance, jnp.zeros((STATE, INNER), jnp.float32), (step, xfloat, bmat, cmat))
    y_out = (outputs + skip[None, :] * xfloat).astype(jnp.bfloat16)
    y_out = lax.optimization_barrier(y_out)
    return (y_out.astype(jnp.float32) * jax.nn.silu(gate_input.astype(jnp.float32))).astype(jnp.bfloat16)
```

```python
import functools

import jax
import jax.numpy as jnp
from jax import lax
from jax.experimental import pallas as pl
from jax.experimental.pallas import tpu as pltpu
from jax.sharding import PartitionSpec as P

LOG2E = 1.4426950408889634
HALO = 8


def conv_kernel(width, x_ref, halo_ref, w_ref, b_ref, xw_ref, xc_ref, part_ref, prev):
    rows, chans = x_ref.shape
    chunk = min(chans, 256)

    @pl.when(pl.program_id(1) == 0)
    def _():
        prev[...] = halo_ref[0]

    for start in range(0, chans, chunk):
        sl = slice(start, start + chunk)
        cur = x_ref[:, sl].astype(jnp.float32)
        ext = jnp.concatenate([prev[:, sl], cur], 0)
        total = b_ref[:, sl] + jnp.zeros((rows, chunk), jnp.float32)
        for tap in range(width):
            low = HALO - width + 1 + tap
            total = total + w_ref[tap : tap + 1, sl] * ext[low : low + rows]
        xc_ref[:, sl] = (total / (1.0 + jnp.exp(-total))).astype(jnp.bfloat16)
        prev[:, sl] = cur[rows - HALO :]
    part_ref[...] = jnp.dot(xc_ref[...], xw_ref[...], preferred_element_type=jnp.float32)


def conv_project(arrived, halo, weight, bias, x_weight, parts, block):
    total, chans = arrived.shape
    steps = total // parts // block
    cols = x_weight.shape[1]
    width = weight.shape[0]
    whole = lambda p, i: (0, 0)
    return pl.pallas_call(
        functools.partial(conv_kernel, width),
        grid=(parts, steps),
        in_specs=[
            pl.BlockSpec((block, chans), lambda p, i: (p * steps + i, 0)),
            pl.BlockSpec((1, HALO, chans), lambda p, i: (p, 0, 0)),
            pl.BlockSpec((width, chans), whole),
            pl.BlockSpec((1, chans), whole),
            pl.BlockSpec((chans, cols), whole),
        ],
        out_specs=[
            pl.BlockSpec((block, chans), lambda p, i: (p * steps + i, 0)),
            pl.BlockSpec((block, cols), lambda p, i: (p * steps + i, 0)),
        ],
        out_shape=[
            jax.ShapeDtypeStruct((total, chans), jnp.bfloat16),
            jax.ShapeDtypeStruct((total, cols), jnp.float32),
        ],
        scratch_shapes=[pltpu.VMEM((HALO, chans), jnp.float32)],
        name="conv_project",
    )(arrived, halo, weight.astype(jnp.float32), bias.astype(jnp.float32)[None, :], x_weight)


def scan_kernel(
    states, xc_ref, nm_ref, bc_ref, dtw_ref, dtb_ref, rate_ref, skip_ref, h0_ref, y_ref, st, dr, ys, hs
):
    rows, chans = xc_ref.shape
    group = chans // 128

    @pl.when(pl.program_id(1) == 0)
    def _():
        hs[...] = h0_ref[0]

    raw = jnp.dot(nm_ref[...], dtw_ref[...], preferred_element_type=jnp.float32) + dtb_ref[...]
    step = jnp.maximum(raw, 0.0) + jnp.log1p(jnp.exp(-jnp.abs(raw)))
    drive = step * xc_ref[...].astype(jnp.float32)
    for j in range(group):
        st[pl.ds(j, rows, stride=group), :] = step[:, j * 128 : (j + 1) * 128]
        dr[pl.ds(j, rows, stride=group), :] = drive[:, j * 128 : (j + 1) * 128]

    rates = [rate_ref[n * group : (n + 1) * group, :] for n in range(states)]

    def advance(t, hidden):
        at = pl.ds(pl.multiple_of(t * group, group), group)
        s = st[at, :]
        d = dr[at, :]
        base = t * (2 * states)
        after = []
        sums = [None, None]
        for n in range(states):
            h = jnp.exp2(s * rates[n]) * hidden[n] + bc_ref[0, 0, base + n] * d
            after.append(h)
            term = bc_ref[0, 0, base + states + n] * h
            sums[n % 2] = term if sums[n % 2] is None else sums[n % 2] + term
        ys[at, :] = sums[0] + sums[1]
        return tuple(after)

    hidden = tuple(hs[n * group : (n + 1) * group, :] for n in range(states))
    hidden = lax.fori_loop(0, rows, advance, hidden, unroll=4)
    for n in range(states):
        hs[n * group : (n + 1) * group, :] = hidden[n]
    for j in range(group):
        sl = slice(j * 128, (j + 1) * 128)
        y = ys[pl.ds(j, rows, stride=group), :] + skip_ref[:, sl] * xc_ref[:, sl].astype(jnp.float32)
        y_ref[:, sl] = y.astype(jnp.bfloat16)


def scan(xc, normed, bc, dt_weight, dt_bias, rate2, skip, start, parts, block):
    total, chans = xc.shape
    states2 = bc.shape[1]
    states = states2 // 2
    group = chans // 128
    steps = total // parts // block
    rank = normed.shape[1]
    whole = lambda p, i: (0, 0)
    tile = lambda p, i: (p * steps + i, 0)
    return pl.pallas_call(
        functools.partial(scan_kernel, states),
        grid=(parts, steps),
        in_specs=[
            pl.BlockSpec((block, chans), tile),
            pl.BlockSpec((block, rank), tile),
            pl.BlockSpec(
                (1, 1, block * states2), lambda p, i: (p * steps + i, 0, 0), memory_space=pltpu.SMEM
            ),
            pl.BlockSpec((rank, chans), whole),
            pl.BlockSpec((1, chans), whole),
            pl.BlockSpec((states * group, 128), whole),
            pl.BlockSpec((1, chans), whole),
            pl.BlockSpec((1, states * group, 128), lambda p, i: (p, 0, 0)),
        ],
        out_specs=pl.BlockSpec((block, chans), tile),
        out_shape=jax.ShapeDtypeStruct((total, chans), jnp.bfloat16),
        scratch_shapes=[
            pltpu.VMEM((block * group, 128), jnp.float32),
            pltpu.VMEM((block * group, 128), jnp.float32),
            pltpu.VMEM((block * group, 128), jnp.float32),
            pltpu.VMEM((states * group, 128), jnp.float32),
        ],
        name="selective_scan",
    )(
        xc,
        normed,
        bc.reshape(parts * steps, 1, block * states2),
        dt_weight,
        dt_bias[None, :],
        rate2.reshape(states * group, 128),
        skip[None, :],
        start,
    )


def local(
    conv_input,
    gate_input,
    conv_weight,
    conv_bias,
    x_weight,
    dt_gain,
    dt_weight,
    dt_bias,
    a_log,
    skip,
):
    rank, chans = dt_weight.shape
    states = a_log.shape[0]
    rows = conv_input.shape[0]
    arrived = lax.all_to_all(conv_input, "seq", split_axis=1, concat_axis=0, tiled=True)
    halo = jnp.zeros((1, HALO, chans), jnp.float32)
    conv_out, partial_value = conv_project(
        arrived, halo, conv_weight, conv_bias, x_weight, 1, rows
    )
    shares = lax.all_to_all(
        partial_value.reshape(-1, rows, partial_value.shape[1]), "seq", split_axis=0, concat_axis=0
    )
    proj = jnp.sum(shares, axis=0)
    dt_low = proj[:, :rank]
    bc = proj[:, rank:]
    normed = (
        dt_low
        * lax.rsqrt(jnp.mean(dt_low * dt_low, axis=1, keepdims=True) + 1e-06)
        * dt_gain[None, :]
    ).astype(jnp.bfloat16)
    high = lax.reduce_precision(bc, 8, 7)
    low = (bc - high).astype(jnp.bfloat16)
    packed = jnp.concatenate([normed, high.astype(jnp.bfloat16), low], 1)
    everyone = lax.all_gather(packed, "seq", axis=0, tiled=True)
    normed_all = everyone[:, :rank]
    bc_all = everyone[:, rank : rank + 2 * states].astype(jnp.float32) + everyone[
        :, rank + 2 * states :
    ].astype(jnp.float32)
    rate2 = -jnp.exp(a_log) * LOG2E
    start = jnp.zeros((1, states * chans // 128, 128), jnp.float32)
    y_out = scan(conv_out, normed_all, bc_all, dt_weight, dt_bias, rate2, skip, start, 1, rows)
    returned = lax.all_to_all(y_out, "seq", split_axis=0, concat_axis=1, tiled=True)
    return (returned.astype(jnp.float32) * jax.nn.silu(gate_input.astype(jnp.float32))).astype(
        jnp.bfloat16
    )


def solution(mesh):
    return jax.shard_map(
        local,
        mesh=mesh,
        in_specs=(
            P(("batch", "seq"), None),
            P(("batch", "seq"), None),
            P(None, "seq"),
            P("seq"),
            P("seq", None),
            P(),
            P(None, "seq"),
            P("seq"),
            P(None, "seq"),
            P("seq"),
        ),
        out_specs=P(("batch", "seq"), None),
        check_vma=False,
    )
```

```python
import functools

import jax
import jax.numpy as jnp
from jax import lax
from jax.experimental import pallas as pl
from jax.experimental.pallas import tpu as pltpu
from jax.sharding import Mesh
from jax.sharding import PartitionSpec as P

LOG2E = 1.4426950408889634
HALO = 8


def conv_kernel(width, x_ref, halo_ref, w_ref, b_ref, xw_ref, xc_ref, part_ref, prev):
    rows, chans = x_ref.shape
    chunk = min(chans, 256)

    @pl.when(pl.program_id(1) == 0)
    def _():
        prev[...] = halo_ref[0]

    for start in range(0, chans, chunk):
        sl = slice(start, start + chunk)
        cur = x_ref[:, sl].astype(jnp.float32)
        ext = jnp.concatenate([prev[:, sl], cur], 0)
        total = b_ref[:, sl] + jnp.zeros((rows, chunk), jnp.float32)
        for tap in range(width):
            low = HALO - width + 1 + tap
            total = total + w_ref[tap : tap + 1, sl] * ext[low : low + rows]
        xc_ref[:, sl] = (total / (1.0 + jnp.exp(-total))).astype(jnp.bfloat16)
        prev[:, sl] = cur[rows - HALO :]
    part_ref[...] = jnp.dot(xc_ref[...], xw_ref[...], preferred_element_type=jnp.float32)


def conv_project(arrived, halo, weight, bias, x_weight, parts, block):
    total, chans = arrived.shape
    steps = total // parts // block
    cols = x_weight.shape[1]
    width = weight.shape[0]
    whole = lambda p, i: (0, 0)
    return pl.pallas_call(
        functools.partial(conv_kernel, width),
        grid=(parts, steps),
        in_specs=[
            pl.BlockSpec((block, chans), lambda p, i: (p * steps + i, 0)),
            pl.BlockSpec((1, HALO, chans), lambda p, i: (p, 0, 0)),
            pl.BlockSpec((width, chans), whole),
            pl.BlockSpec((1, chans), whole),
            pl.BlockSpec((chans, cols), whole),
        ],
        out_specs=[
            pl.BlockSpec((block, chans), lambda p, i: (p * steps + i, 0)),
            pl.BlockSpec((block, cols), lambda p, i: (p * steps + i, 0)),
        ],
        out_shape=[
            jax.ShapeDtypeStruct((total, chans), jnp.bfloat16),
            jax.ShapeDtypeStruct((total, cols), jnp.float32),
        ],
        scratch_shapes=[pltpu.VMEM((HALO, chans), jnp.float32)],
        name="conv_project",
    )(arrived, halo, weight.astype(jnp.float32), bias.astype(jnp.float32)[None, :], x_weight)


def prepare_kernel(
    states, xc_ref, nm_ref, bc_ref, dtw_ref, dtb_ref, rate_ref, st, dr, end_ref, sum_ref
):
    rows, chans = xc_ref.shape
    group = chans // 128

    @pl.when(pl.program_id(1) == 0)
    def _():
        end_ref[...] = jnp.zeros_like(end_ref)
        sum_ref[...] = jnp.zeros_like(sum_ref)

    raw = jnp.dot(nm_ref[...], dtw_ref[...], preferred_element_type=jnp.float32) + dtb_ref[...]
    step = jnp.maximum(raw, 0.0) + jnp.log1p(jnp.exp(-jnp.abs(raw)))
    drive = step * xc_ref[...].astype(jnp.float32)
    for j in range(group):
        st[pl.ds(j, rows, stride=group), :] = step[:, j * 128 : (j + 1) * 128]
        dr[pl.ds(j, rows, stride=group), :] = drive[:, j * 128 : (j + 1) * 128]

    rates = [rate_ref[n * group : (n + 1) * group, :] for n in range(states)]

    def advance(t, carry):
        at = pl.ds(pl.multiple_of(t * group, group), group)
        s = st[at, :]
        d = dr[at, :]
        base = t * (2 * states)
        after = [
            jnp.exp2(s * rates[n]) * carry[n] + bc_ref[0, 0, base + n] * d for n in range(states)
        ]
        return tuple(after) + (carry[states] + s,)

    carry = tuple(end_ref[0, n * group : (n + 1) * group, :] for n in range(states))
    carry = lax.fori_loop(0, rows, advance, carry + (sum_ref[0],), unroll=4)
    for n in range(states):
        end_ref[0, n * group : (n + 1) * group, :] = carry[n]
    sum_ref[0] = carry[states]


def prepare(xc, normed, bc, dt_weight, dt_bias, rate2, first, parts, steps, block):
    chans = xc.shape[1]
    states2 = bc.shape[2] // block
    states = states2 // 2
    group = chans // 128
    rank = normed.shape[1]
    whole = lambda p, i: (0, 0)
    tile = lambda p, i: ((first + p) * steps + i, 0)
    mine = lambda p, i: (p * steps + i, 0)
    total = parts * steps * block
    return pl.pallas_call(
        functools.partial(prepare_kernel, states),
        grid=(parts, steps),
        in_specs=[
            pl.BlockSpec((block, chans), tile),
            pl.BlockSpec((block, rank), tile),
            pl.BlockSpec(
                (1, 1, block * states2),
                lambda p, i: ((first + p) * steps + i, 0, 0),
                memory_space=pltpu.SMEM,
            ),
            pl.BlockSpec((rank, chans), whole),
            pl.BlockSpec((1, chans), whole),
            pl.BlockSpec((states * group, 128), whole),
        ],
        out_specs=[
            pl.BlockSpec((block * group, 128), mine),
            pl.BlockSpec((block * group, 128), mine),
            pl.BlockSpec((1, states * group, 128), lambda p, i: (p, 0, 0)),
            pl.BlockSpec((1, group, 128), lambda p, i: (p, 0, 0)),
        ],
        out_shape=[
            jax.ShapeDtypeStruct((total * group, 128), jnp.float32),
            jax.ShapeDtypeStruct((total * group, 128), jnp.float32),
            jax.ShapeDtypeStruct((parts, states * group, 128), jnp.float32),
            jax.ShapeDtypeStruct((parts, group, 128), jnp.float32),
        ],
        cost_estimate=pl.CostEstimate(
            flops=total * chans * (2 * rank + 5 * states),
            bytes_accessed=total * chans * 10,
            transcendentals=total * chans * states,
        ),
        name="prepare",
    )(xc, normed, bc, dt_weight, dt_bias, rate2)


def scan_kernel(states, xc_ref, st, dr, bc_ref, rate_ref, skip_ref, h0_ref, y_ref, ys, hs):
    rows, chans = xc_ref.shape
    group = chans // 128

    @pl.when(pl.program_id(1) == 0)
    def _():
        hs[...] = h0_ref[0].astype(jnp.float32)

    rates = [rate_ref[n * group : (n + 1) * group, :] for n in range(states)]

    def advance(t, hidden):
        at = pl.ds(pl.multiple_of(t * group, group), group)
        s = st[at, :]
        d = dr[at, :]
        base = t * (2 * states)
        after = []
        sums = [None, None]
        for n in range(states):
            h = jnp.exp2(s * rates[n]) * hidden[n] + bc_ref[0, 0, base + n] * d
            after.append(h)
            term = bc_ref[0, 0, base + states + n] * h
            sums[n % 2] = term if sums[n % 2] is None else sums[n % 2] + term
        ys[at, :] = sums[0] + sums[1]
        return tuple(after)

    hidden = tuple(hs[n * group : (n + 1) * group, :] for n in range(states))
    hidden = lax.fori_loop(0, rows, advance, hidden, unroll=4)
    for n in range(states):
        hs[n * group : (n + 1) * group, :] = hidden[n]
    for j in range(group):
        sl = slice(j * 128, (j + 1) * 128)
        y = ys[pl.ds(j, rows, stride=group), :] + skip_ref[:, sl] * xc_ref[:, sl].astype(jnp.float32)
        y_ref[:, sl] = y.astype(jnp.bfloat16)


def scan(xc, st, dr, bc, rate2, skip, start, first, parts, steps, block):
    chans = xc.shape[1]
    states2 = bc.shape[2] // block
    states = states2 // 2
    group = chans // 128
    whole = lambda p, i: (0, 0)
    mine = lambda p, i: (p * steps + i, 0)
    total = parts * steps * block
    return pl.pallas_call(
        functools.partial(scan_kernel, states),
        grid=(parts, steps),
        in_specs=[
            pl.BlockSpec((block, chans), lambda p, i: ((first + p) * steps + i, 0)),
            pl.BlockSpec((block * group, 128), mine),
            pl.BlockSpec((block * group, 128), mine),
            pl.BlockSpec(
                (1, 1, block * states2),
                lambda p, i: ((first + p) * steps + i, 0, 0),
                memory_space=pltpu.SMEM,
            ),
            pl.BlockSpec((states * group, 128), whole),
            pl.BlockSpec((1, chans), whole),
            pl.BlockSpec((1, states * group, 128), lambda p, i: (p, 0, 0)),
        ],
        out_specs=pl.BlockSpec((block, chans), mine),
        out_shape=jax.ShapeDtypeStruct((total, chans), jnp.bfloat16),
        scratch_shapes=[
            pltpu.VMEM((block * group, 128), jnp.float32),
            pltpu.VMEM((states * group, 128), jnp.float32),
        ],
        cost_estimate=pl.CostEstimate(
            flops=total * chans * 7 * states,
            bytes_accessed=total * chans * 12,
            transcendentals=total * chans * states,
        ),
        name="selective_scan",
    )(xc, st, dr, bc, rate2, skip, start)


PLANE = ("core", "x", "y")
SPLITS = 2


def local(
    sizes,
    conv_input,
    gate_input,
    conv_weight,
    conv_bias,
    x_weight,
    dt_gain,
    dt_weight,
    dt_bias,
    a_log,
    skip,
):
    depth, parts = sizes
    rank, chans = dt_weight.shape
    states = a_log.shape[0]
    rows = conv_input.shape[0]
    group = chans // 128
    cores = parts // lax.axis_size("x")
    place = lambda z, b: z * parts + b % (parts // cores) * cores + b // (parts // cores)
    swap = [(place(a, b), place(b, a)) for a in range(depth) for b in range(parts)]
    move = lambda v: lax.ppermute(v, ("z", "x", "core"), swap)
    following = [(z, z + 1) for z in range(depth - 1)]
    onward = lambda v: lax.ppermute(v, "z", following)

    conv_pack = move(jnp.concatenate([conv_weight, conv_bias[None, :]], 0))
    x_weight = move(x_weight)
    dt_weight = move(dt_weight)
    scan_pack = move(jnp.concatenate([a_log, dt_bias[None, :], skip[None, :]], 0))
    width = conv_weight.shape[0]
    conv_weight, conv_bias = conv_pack[:width], conv_pack[width]

    arrived = lax.all_to_all(conv_input, PLANE, split_axis=1, concat_axis=0, tiled=True)
    span = arrived.shape[0] // parts
    halo = onward(arrived.reshape(parts, span, chans)[:, span - HALO :]).astype(jnp.float32)
    conv_out, partial_value = conv_project(
        arrived, halo, conv_weight, conv_bias, x_weight, parts, rows
    )
    shares = lax.all_to_all(
        partial_value.reshape(-1, rows, partial_value.shape[1]), PLANE, split_axis=0, concat_axis=0
    )
    proj = jnp.sum(shares, axis=0)
    dt_low = proj[:, :rank]
    bc = proj[:, rank:]
    normed = (
        dt_low
        * lax.rsqrt(jnp.mean(dt_low * dt_low, axis=1, keepdims=True) + 1e-06)
        * dt_gain[None, :]
    ).astype(jnp.bfloat16)
    high = lax.reduce_precision(bc, 8, 7)
    low = (bc - high).astype(jnp.bfloat16)
    packed = jnp.concatenate([normed, high.astype(jnp.bfloat16), low], 1)
    everyone = lax.all_gather(packed, PLANE, axis=0, tiled=True)
    normed_all = everyone[:, :rank]
    bc_all = everyone[:, rank : rank + 2 * states].astype(jnp.float32) + everyone[
        :, rank + 2 * states :
    ].astype(jnp.float32)
    bc_all = bc_all.reshape(-1, 1, rows * 2 * states)
    rate2 = (-jnp.exp(scan_pack[:states]) * LOG2E).reshape(states * group, 128)
    dt_bias, skip = scan_pack[states : states + 1], scan_pack[states + 1 :]
    steps = span // rows
    some = parts // SPLITS
    pieces = []
    for first in range(0, parts, some):
        st, dr, ends, sums = prepare(
            conv_out, normed_all, bc_all, dt_weight, dt_bias, rate2, first, some, steps, rows
        )
        decay = jnp.exp2(
            sums[:, None] * rate2.reshape(1, states, group, 128)
        ).reshape(ends.shape)
        start = onward(ends.astype(jnp.bfloat16))
        for _ in range(depth - 2):
            start = onward((decay * start.astype(jnp.float32) + ends).astype(jnp.bfloat16))
        pieces.append(
            scan(conv_out, st, dr, bc_all, rate2, skip, start, first, some, steps, rows)
        )
    y_out = jnp.concatenate(pieces, 0)
    returned = lax.all_to_all(y_out, PLANE, split_axis=0, concat_axis=1, tiled=True)
    return (returned.astype(jnp.float32) * jax.nn.silu(gate_input.astype(jnp.float32))).astype(
        jnp.bfloat16
    )


def solution(mesh):
    seq, batch = mesh.shape["seq"], mesh.shape["batch"]
    cores = 2
    grid = Mesh(
        mesh.devices.reshape(batch, seq // batch, batch // cores, cores), ("z", "y", "x", "core")
    )
    seqs = ("z", "y")
    rows = P(("x", "core", "z", "y"), None)
    return jax.shard_map(
        functools.partial(local, (batch, batch)),
        mesh=grid,
        in_specs=(
            rows,
            rows,
            P(None, seqs),
            P(seqs),
            P(seqs, None),
            P(),
            P(None, seqs),
            P(seqs),
            P(None, seqs),
            P(seqs),
        ),
        out_specs=rows,
        check_vma=False,
    )
```

```python
import functools

import jax
import jax.numpy as jnp
from jax import lax
from jax.experimental import pallas as pl
from jax.experimental.pallas import tpu as pltpu
from jax.sharding import Mesh
from jax.sharding import PartitionSpec as P

LOG2E = 1.4426950408889634
HALO = 8


MESH = pl.DeviceIdType.MESH


def pack(wide, exact):
    high = exact.astype(jnp.bfloat16)
    low = (exact - high.astype(jnp.float32)).astype(jnp.bfloat16)
    rest = -(2 * exact.shape[1]) % 128
    pieces = [wide.astype(jnp.bfloat16), high, low]
    if rest:
        pieces.append(jnp.zeros((exact.shape[0], rest), jnp.bfloat16))
    return jnp.concatenate(pieces, 1)


def place():
    x, y, core = lax.axis_index("x"), lax.axis_index("y"), lax.axis_index("core")
    return (core * lax.axis_size("x") + x) * lax.axis_size("y") + y


def device(index):
    ys, xs = lax.axis_size("y"), lax.axis_size("x")
    part = index // ys
    return {"x": lax.rem(part, xs), "y": lax.rem(index, ys), "core": part // xs}


def greet(peers):
    me = place()
    barrier = pltpu.get_barrier_semaphore()
    for k in range(1, peers):
        pl.semaphore_signal(
            barrier, inc=1, device_id=device(lax.rem(me + k, peers)), device_id_type=MESH
        )
    pl.semaphore_wait(barrier, peers - 1)
    return me


def reduce_kernel(peers, rank, states2, part_ref, gain_ref, out_ref, got, send_sem, recv_sem):
    rows = got.shape[1]
    me = greet(peers)
    spread = []
    for k in range(1, peers):
        other = lax.rem(me + k, peers)
        copy = pltpu.make_async_remote_copy(
            src_ref=part_ref.at[pl.ds(pl.multiple_of(other * rows, rows), rows)],
            dst_ref=got.at[k],
            send_sem=send_sem.at[0, k],
            recv_sem=recv_sem.at[0, k],
            device_id=device(other),
            device_id_type=MESH,
        )
        copy.start()
        spread.append(copy)
    mine = pl.ds(pl.multiple_of(me * rows, rows), rows)
    total = part_ref[mine, :].astype(jnp.float32)
    for k in range(1, peers):
        spread[k - 1].wait_recv()
        total = total + got[k].astype(jnp.float32)
    low = total[:, :rank]
    exact = total[:, rank : rank + states2] + total[:, rank + states2 : rank + 2 * states2]
    normed = low * lax.rsqrt(jnp.mean(low * low, axis=1, keepdims=True) + 1e-06) * gain_ref[...]
    out_ref[mine, :] = pack(normed, exact)
    gather = []
    for k in range(1, peers):
        copy = pltpu.make_async_remote_copy(
            src_ref=out_ref.at[mine],
            dst_ref=out_ref.at[mine],
            send_sem=send_sem.at[1, k],
            recv_sem=recv_sem.at[1, k],
            device_id=device(lax.rem(me + k, peers)),
            device_id_type=MESH,
        )
        copy.start()
        gather.append(copy)
    for k in range(1, peers):
        spread[k - 1].wait_send()
        gather[k - 1].wait()


def reduce_norm(partial, gain, peers, rank, states2):
    total, cols = partial.shape
    return pl.pallas_call(
        functools.partial(reduce_kernel, peers, rank, states2),
        in_specs=[pl.BlockSpec(memory_space=pltpu.VMEM)] * 2,
        out_specs=pl.BlockSpec(memory_space=pltpu.VMEM),
        out_shape=jax.ShapeDtypeStruct((total, cols), jnp.bfloat16),
        scratch_shapes=[
            pltpu.VMEM((peers, total // peers, cols), jnp.bfloat16),
            pltpu.SemaphoreType.DMA((2, peers)),
            pltpu.SemaphoreType.DMA((2, peers)),
        ],
        compiler_params=pltpu.CompilerParams(collective_id=0, has_side_effects=True),
        name="reduce_norm",
    )(partial, gain[None, :])


def conv_kernel(width, rank, x_ref, halo_ref, w_ref, b_ref, xw_ref, xc_ref, part_ref, prev):
    rows, chans = x_ref.shape
    chunk = min(chans, 256)

    @pl.when(pl.program_id(1) == 0)
    def _():
        prev[...] = halo_ref[0]

    for start in range(0, chans, chunk):
        sl = slice(start, start + chunk)
        cur = x_ref[:, sl].astype(jnp.float32)
        ext = jnp.concatenate([prev[:, sl], cur], 0)
        total = b_ref[:, sl] + jnp.zeros((rows, chunk), jnp.float32)
        for tap in range(width):
            low = HALO - width + 1 + tap
            total = total + w_ref[tap : tap + 1, sl] * ext[low : low + rows]
        xc_ref[:, sl] = (total / (1.0 + jnp.exp(-total))).astype(jnp.bfloat16)
        prev[:, sl] = cur[rows - HALO :]
    part = jnp.dot(xc_ref[...], xw_ref[...], preferred_element_type=jnp.float32)
    part_ref[...] = pack(part[:, :rank], part[:, rank:])


def conv_project(arrived, halo, weight, bias, x_weight, parts, block, rank):
    total, chans = arrived.shape
    steps = total // parts // block
    cols = x_weight.shape[1]
    width = weight.shape[0]
    packed = rank + -(-2 * (cols - rank) // 128) * 128
    whole = lambda p, i: (0, 0)
    return pl.pallas_call(
        functools.partial(conv_kernel, width, rank),
        grid=(parts, steps),
        in_specs=[
            pl.BlockSpec((block, chans), lambda p, i: (p * steps + i, 0)),
            pl.BlockSpec((1, HALO, chans), lambda p, i: (p, 0, 0)),
            pl.BlockSpec((width, chans), whole),
            pl.BlockSpec((1, chans), whole),
            pl.BlockSpec((chans, cols), whole),
        ],
        out_specs=[
            pl.BlockSpec((block, chans), lambda p, i: (p * steps + i, 0)),
            pl.BlockSpec((block, packed), lambda p, i: (p * steps + i, 0)),
        ],
        out_shape=[
            jax.ShapeDtypeStruct((total, chans), jnp.bfloat16),
            jax.ShapeDtypeStruct((total, packed), jnp.bfloat16),
        ],
        scratch_shapes=[pltpu.VMEM((HALO, chans), jnp.float32)],
        name="conv_project",
    )(arrived, halo, weight.astype(jnp.float32), bias.astype(jnp.float32)[None, :], x_weight)


def prepare_kernel(
    states, xc_ref, nm_ref, bc_ref, dtw_ref, dtb_ref, rate_ref, st, dr, end_ref, sum_ref
):
    rows, chans = xc_ref.shape
    group = chans // 128

    @pl.when(pl.program_id(1) == 0)
    def _():
        end_ref[...] = jnp.zeros_like(end_ref)
        sum_ref[...] = jnp.zeros_like(sum_ref)

    raw = jnp.dot(nm_ref[...], dtw_ref[...], preferred_element_type=jnp.float32) + dtb_ref[...]
    step = jnp.maximum(raw, 0.0) + jnp.log1p(jnp.exp(-jnp.abs(raw)))
    drive = step * xc_ref[...].astype(jnp.float32)
    for j in range(group):
        st[pl.ds(j, rows, stride=group), :] = step[:, j * 128 : (j + 1) * 128]
        dr[pl.ds(j, rows, stride=group), :] = drive[:, j * 128 : (j + 1) * 128]

    rates = [rate_ref[n * group : (n + 1) * group, :] for n in range(states)]

    def advance(t, carry):
        at = pl.ds(pl.multiple_of(t * group, group), group)
        s = st[at, :]
        d = dr[at, :]
        base = t * (2 * states)
        after = [
            jnp.exp2(s * rates[n]) * carry[n] + bc_ref[0, 0, base + n] * d for n in range(states)
        ]
        return tuple(after) + (carry[states] + s,)

    carry = tuple(end_ref[0, n * group : (n + 1) * group, :] for n in range(states))
    carry = lax.fori_loop(0, rows, advance, carry + (sum_ref[0],), unroll=4)
    for n in range(states):
        end_ref[0, n * group : (n + 1) * group, :] = carry[n]
    sum_ref[0] = carry[states]


def prepare(xc, normed, bc, dt_weight, dt_bias, rate2, first, parts, steps, block):
    chans = xc.shape[1]
    states2 = bc.shape[2] // block
    states = states2 // 2
    group = chans // 128
    rank = normed.shape[1]
    whole = lambda p, i: (0, 0)
    tile = lambda p, i: ((first + p) * steps + i, 0)
    mine = lambda p, i: (p * steps + i, 0)
    total = parts * steps * block
    return pl.pallas_call(
        functools.partial(prepare_kernel, states),
        grid=(parts, steps),
        in_specs=[
            pl.BlockSpec((block, chans), tile),
            pl.BlockSpec((block, rank), tile),
            pl.BlockSpec(
                (1, 1, block * states2),
                lambda p, i: ((first + p) * steps + i, 0, 0),
                memory_space=pltpu.SMEM,
            ),
            pl.BlockSpec((rank, chans), whole),
            pl.BlockSpec((1, chans), whole),
            pl.BlockSpec((states * group, 128), whole),
        ],
        out_specs=[
            pl.BlockSpec((block * group, 128), mine),
            pl.BlockSpec((block * group, 128), mine),
            pl.BlockSpec((1, states * group, 128), lambda p, i: (p, 0, 0)),
            pl.BlockSpec((1, group, 128), lambda p, i: (p, 0, 0)),
        ],
        out_shape=[
            jax.ShapeDtypeStruct((total * group, 128), jnp.float32),
            jax.ShapeDtypeStruct((total * group, 128), jnp.float32),
            jax.ShapeDtypeStruct((parts, states * group, 128), jnp.float32),
            jax.ShapeDtypeStruct((parts, group, 128), jnp.float32),
        ],
        cost_estimate=pl.CostEstimate(
            flops=total * chans * (2 * rank + 5 * states),
            bytes_accessed=total * chans * 10,
            transcendentals=total * chans * states,
        ),
        name="prepare",
    )(xc, normed, bc, dt_weight, dt_bias, rate2)


def scan_kernel(
    states, parts, peers, xc_ref, st, dr, bc_ref, rate_ref, skip_ref, h0_ref, out_ref,
    ybuf, ys, hs, send_sem, recv_sem, own_sem,
):
    total, chans = xc_ref.shape
    group = chans // 128
    rows = total // peers
    steps = total // parts // rows
    xs = lax.axis_size("x")
    cores = parts // xs
    x = lax.axis_index("x")
    me = greet(peers)
    columns = out_ref.at[:, pl.ds(pl.multiple_of(me * chans, chans), chans)]
    rates = [rate_ref[n * group : (n + 1) * group, :] for n in range(states)]

    def send(block):
        away = lax.rem(block - me + peers, peers)
        return pltpu.make_async_remote_copy(
            src_ref=ybuf.at[block],
            dst_ref=columns,
            send_sem=send_sem.at[away],
            recv_sem=recv_sem.at[away],
            device_id=device(block),
            device_id_type=MESH,
        )

    own = pltpu.make_async_copy(ybuf.at[me], columns, own_sem)

    def one_block(place_in_order, _):
        turn, i = place_in_order // steps, lax.rem(place_in_order, steps)
        part = lax.rem(turn, cores) * xs + lax.rem(x + 1 + turn // cores, xs)
        block = part * steps + i
        base_row = pl.multiple_of(block * rows, rows)

        @pl.when(i == 0)
        def _():
            hs[...] = h0_ref[part].astype(jnp.float32)

        def advance(t, hidden):
            at = pl.ds(pl.multiple_of((base_row + t) * group, group), group)
            s = st[at, :]
            d = dr[at, :]
            base = (base_row + t) * (2 * states)
            after = []
            sums = [None, None]
            for n in range(states):
                h = jnp.exp2(s * rates[n]) * hidden[n] + bc_ref[base + n] * d
                after.append(h)
                term = bc_ref[base + states + n] * h
                sums[n % 2] = term if sums[n % 2] is None else sums[n % 2] + term
            ys[pl.ds(pl.multiple_of(t * group, group), group), :] = sums[0] + sums[1]
            return tuple(after)

        hidden = tuple(hs[n * group : (n + 1) * group, :] for n in range(states))
        hidden = lax.fori_loop(0, rows, advance, hidden, unroll=4)
        for n in range(states):
            hs[n * group : (n + 1) * group, :] = hidden[n]
        for j in range(group):
            sl = slice(j * 128, (j + 1) * 128)
            skipped = skip_ref[:, sl] * xc_ref[pl.ds(base_row, rows), sl].astype(jnp.float32)
            y = ys[pl.ds(j, rows, stride=group), :] + skipped
            ybuf[block, :, sl] = y.astype(jnp.bfloat16)

        @pl.when(block == me)
        def _():
            own.start()

        @pl.when(block != me)
        def _():
            send(block).start()

        return 0

    lax.fori_loop(0, peers, one_block, 0)
    own.wait()
    for k in range(1, peers):
        send(lax.rem(me + k, peers)).wait()


def scan(xc, st, dr, bc, rate2, skip, start, parts, peers):
    total, chans = xc.shape
    states = bc.shape[0] // total // 2
    group = chans // 128
    rows = total // peers
    vmem = pl.BlockSpec(memory_space=pltpu.VMEM)
    return pl.pallas_call(
        functools.partial(scan_kernel, states, parts, peers),
        in_specs=[vmem, vmem, vmem, pl.BlockSpec(memory_space=pltpu.SMEM), vmem, vmem, vmem],
        out_specs=pl.BlockSpec(memory_space=pl.ANY),
        out_shape=jax.ShapeDtypeStruct((rows, peers * chans), jnp.bfloat16),
        scratch_shapes=[
            pltpu.VMEM((peers, rows, chans), jnp.bfloat16),
            pltpu.VMEM((rows * group, 128), jnp.float32),
            pltpu.VMEM((states * group, 128), jnp.float32),
            pltpu.SemaphoreType.DMA((peers,)),
            pltpu.SemaphoreType.DMA((peers,)),
            pltpu.SemaphoreType.DMA,
        ],
        compiler_params=pltpu.CompilerParams(collective_id=1, has_side_effects=True),
        name="selective_scan",
    )(xc, st, dr, bc, rate2, skip, start)


PLANE = ("core", "x", "y")


def local(
    sizes,
    conv_input,
    gate_input,
    conv_weight,
    conv_bias,
    x_weight,
    dt_gain,
    dt_weight,
    dt_bias,
    a_log,
    skip,
):
    depth, parts = sizes
    rank, chans = dt_weight.shape
    states = a_log.shape[0]
    rows = conv_input.shape[0]
    group = chans // 128
    cores = parts // lax.axis_size("x")
    place = lambda z, b: z * parts + b % (parts // cores) * cores + b // (parts // cores)
    swap = [(place(a, b), place(b, a)) for a in range(depth) for b in range(parts)]
    move = lambda v: lax.ppermute(v, ("z", "x", "core"), swap)
    following = [(z, z + 1) for z in range(depth - 1)]
    onward = lambda v: lax.ppermute(v, "z", following)

    conv_pack = move(jnp.concatenate([conv_weight, conv_bias[None, :]], 0))
    x_weight = move(x_weight)
    dt_weight = move(dt_weight)
    scan_pack = move(jnp.concatenate([a_log, dt_bias[None, :], skip[None, :]], 0))
    width = conv_weight.shape[0]
    conv_weight, conv_bias = conv_pack[:width], conv_pack[width]

    arrived = lax.all_to_all(conv_input, PLANE, split_axis=1, concat_axis=0, tiled=True)
    span = arrived.shape[0] // parts
    halo = onward(arrived.reshape(parts, span, chans)[:, span - HALO :]).astype(jnp.float32)
    conv_out, partial_value = conv_project(
        arrived, halo, conv_weight, conv_bias, x_weight, parts, rows, rank
    )
    everyone = reduce_norm(partial_value, dt_gain, arrived.shape[0] // rows, rank, 2 * states)
    normed_all = everyone[:, :rank]
    bc_all = everyone[:, rank : rank + 2 * states].astype(jnp.float32) + everyone[
        :, rank + 2 * states : rank + 4 * states
    ].astype(jnp.float32)
    bc_all = bc_all.reshape(-1, 1, rows * 2 * states)
    rate2 = (-jnp.exp(scan_pack[:states]) * LOG2E).reshape(states * group, 128)
    dt_bias, skip = scan_pack[states : states + 1], scan_pack[states + 1 :]
    steps = span // rows
    st, dr, ends, sums = prepare(
        conv_out, normed_all, bc_all, dt_weight, dt_bias, rate2, 0, parts, steps, rows
    )
    decay = jnp.exp2(sums[:, None] * rate2.reshape(1, states, group, 128)).reshape(ends.shape)
    start = onward(ends.astype(jnp.bfloat16))
    for _ in range(depth - 2):
        start = onward((decay * start.astype(jnp.float32) + ends).astype(jnp.bfloat16))
    returned = scan(
        conv_out, st, dr, bc_all.reshape(-1), rate2, skip, start, parts, arrived.shape[0] // rows
    )
    return (returned.astype(jnp.float32) * jax.nn.silu(gate_input.astype(jnp.float32))).astype(
        jnp.bfloat16
    )


def solution(mesh):
    seq, batch = mesh.shape["seq"], mesh.shape["batch"]
    cores = 2
    grid = Mesh(
        mesh.devices.reshape(batch, seq // batch, batch // cores, cores), ("z", "y", "x", "core")
    )
    seqs = ("z", "y")
    rows = P(("x", "core", "z", "y"), None)
    return jax.shard_map(
        functools.partial(local, (batch, batch)),
        mesh=grid,
        in_specs=(
            rows,
            rows,
            P(None, seqs),
            P(seqs),
            P(seqs, None),
            P(),
            P(None, seqs),
            P(seqs),
            P(None, seqs),
            P(seqs),
        ),
        out_specs=rows,
        check_vma=False,
    )
```

```python
import functools

import jax
import jax.numpy as jnp
from jax import lax
from jax.experimental import pallas as pl
from jax.experimental.pallas import tpu as pltpu
from jax.sharding import Mesh
from jax.sharding import PartitionSpec as P

LOG2E = 1.4426950408889634
HALO = 8


MESH = pl.DeviceIdType.MESH


def pack(wide, exact):
    high = exact.astype(jnp.bfloat16)
    low = (exact - high.astype(jnp.float32)).astype(jnp.bfloat16)
    rest = -(2 * exact.shape[1]) % 128
    pieces = [wide.astype(jnp.bfloat16), high, low]
    if rest:
        pieces.append(jnp.zeros((exact.shape[0], rest), jnp.bfloat16))
    return jnp.concatenate(pieces, 1)


def place():
    x, y, core = lax.axis_index("x"), lax.axis_index("y"), lax.axis_index("core")
    return (core * lax.axis_size("x") + x) * lax.axis_size("y") + y


def device(index):
    ys, xs = lax.axis_size("y"), lax.axis_size("x")
    part = index // ys
    return {"x": lax.rem(part, xs), "y": lax.rem(index, ys), "core": part // xs}


def greet(peers):
    me = place()
    barrier = pltpu.get_barrier_semaphore()
    for k in range(1, peers):
        pl.semaphore_signal(
            barrier, inc=1, device_id=device(lax.rem(me + k, peers)), device_id_type=MESH
        )
    pl.semaphore_wait(barrier, peers - 1)
    return me


def reduce_kernel(peers, rank, states2, part_ref, gain_ref, out_ref, got, send_sem, recv_sem):
    rows = got.shape[1]
    me = greet(peers)
    spread = []
    for k in range(1, peers):
        other = lax.rem(me + k, peers)
        copy = pltpu.make_async_remote_copy(
            src_ref=part_ref.at[pl.ds(pl.multiple_of(other * rows, rows), rows)],
            dst_ref=got.at[k],
            send_sem=send_sem.at[0, k],
            recv_sem=recv_sem.at[0, k],
            device_id=device(other),
            device_id_type=MESH,
        )
        copy.start()
        spread.append(copy)
    mine = pl.ds(pl.multiple_of(me * rows, rows), rows)
    total = part_ref[mine, :].astype(jnp.float32)
    for k in range(1, peers):
        spread[k - 1].wait_recv()
        total = total + got[k].astype(jnp.float32)
    low = total[:, :rank]
    exact = total[:, rank : rank + states2] + total[:, rank + states2 : rank + 2 * states2]
    normed = low * lax.rsqrt(jnp.mean(low * low, axis=1, keepdims=True) + 1e-06) * gain_ref[...]
    out_ref[mine, :] = pack(normed, exact)
    gather = []
    for k in range(1, peers):
        copy = pltpu.make_async_remote_copy(
            src_ref=out_ref.at[mine],
            dst_ref=out_ref.at[mine],
            send_sem=send_sem.at[1, k],
            recv_sem=recv_sem.at[1, k],
            device_id=device(lax.rem(me + k, peers)),
            device_id_type=MESH,
        )
        copy.start()
        gather.append(copy)
    for k in range(1, peers):
        spread[k - 1].wait_send()
        gather[k - 1].wait()


def reduce_norm(partial, gain, peers, rank, states2):
    total, cols = partial.shape
    return pl.pallas_call(
        functools.partial(reduce_kernel, peers, rank, states2),
        in_specs=[pl.BlockSpec(memory_space=pltpu.VMEM)] * 2,
        out_specs=pl.BlockSpec(memory_space=pltpu.VMEM),
        out_shape=jax.ShapeDtypeStruct((total, cols), jnp.bfloat16),
        scratch_shapes=[
            pltpu.VMEM((peers, total // peers, cols), jnp.bfloat16),
            pltpu.SemaphoreType.DMA((2, peers)),
            pltpu.SemaphoreType.DMA((2, peers)),
        ],
        compiler_params=pltpu.CompilerParams(collective_id=0, has_side_effects=True),
        name="reduce_norm",
    )(partial, gain[None, :])


def exchange_kernel(peers, in_ref, out_ref, send_sem, recv_sem):
    rows = in_ref.shape[0]
    chans = out_ref.shape[1]
    me = greet(peers)
    mine = pl.ds(pl.multiple_of(me * rows, rows), rows)
    copies = []
    for k in range(1, peers):
        other = lax.rem(me + k, peers)
        copy = pltpu.make_async_remote_copy(
            src_ref=in_ref.at[:, pl.ds(pl.multiple_of(other * chans, chans), chans)],
            dst_ref=out_ref.at[mine],
            send_sem=send_sem.at[k],
            recv_sem=recv_sem.at[k],
            device_id=device(other),
            device_id_type=MESH,
        )
        copy.start()
        copies.append(copy)
    out_ref[mine, :] = in_ref[:, pl.ds(pl.multiple_of(me * chans, chans), chans)]
    for copy in copies:
        copy.wait()


def exchange(inputs, peers):
    rows, total = inputs.shape
    return pl.pallas_call(
        functools.partial(exchange_kernel, peers),
        in_specs=[pl.BlockSpec(memory_space=pltpu.VMEM)],
        out_specs=pl.BlockSpec(memory_space=pltpu.VMEM),
        out_shape=jax.ShapeDtypeStruct((peers * rows, total // peers), inputs.dtype),
        scratch_shapes=[
            pltpu.SemaphoreType.DMA((peers,)),
            pltpu.SemaphoreType.DMA((peers,)),
        ],
        compiler_params=pltpu.CompilerParams(collective_id=2, has_side_effects=True),
        cost_estimate=pl.CostEstimate(
            flops=0, bytes_accessed=24 * rows * total, transcendentals=0
        ),
        name="exchange",
    )(inputs)


def conv_kernel(width, rank, x_ref, halo_ref, w_ref, b_ref, xw_ref, xc_ref, part_ref, prev):
    rows, chans = x_ref.shape
    chunk = min(chans, 256)

    @pl.when(pl.program_id(1) == 0)
    def _():
        prev[...] = halo_ref[0]

    for start in range(0, chans, chunk):
        sl = slice(start, start + chunk)
        cur = x_ref[:, sl].astype(jnp.float32)
        ext = jnp.concatenate([prev[:, sl], cur], 0)
        total = b_ref[:, sl] + jnp.zeros((rows, chunk), jnp.float32)
        for tap in range(width):
            low = HALO - width + 1 + tap
            total = total + w_ref[tap : tap + 1, sl] * ext[low : low + rows]
        xc_ref[:, sl] = (total / (1.0 + jnp.exp(-total))).astype(jnp.bfloat16)
        prev[:, sl] = cur[rows - HALO :]
    part = jnp.dot(xc_ref[...], xw_ref[...], preferred_element_type=jnp.float32)
    part_ref[...] = pack(part[:, :rank], part[:, rank:])


def conv_project(arrived, halo, weight, bias, x_weight, parts, block, rank):
    total, chans = arrived.shape
    steps = total // parts // block
    cols = x_weight.shape[1]
    width = weight.shape[0]
    packed = rank + -(-2 * (cols - rank) // 128) * 128
    whole = lambda p, i: (0, 0)
    return pl.pallas_call(
        functools.partial(conv_kernel, width, rank),
        grid=(parts, steps),
        in_specs=[
            pl.BlockSpec((block, chans), lambda p, i: (p * steps + i, 0)),
            pl.BlockSpec((1, HALO, chans), lambda p, i: (p, 0, 0)),
            pl.BlockSpec((width, chans), whole),
            pl.BlockSpec((1, chans), whole),
            pl.BlockSpec((chans, cols), whole),
        ],
        out_specs=[
            pl.BlockSpec((block, chans), lambda p, i: (p * steps + i, 0)),
            pl.BlockSpec((block, packed), lambda p, i: (p * steps + i, 0)),
        ],
        out_shape=[
            jax.ShapeDtypeStruct((total, chans), jnp.bfloat16),
            jax.ShapeDtypeStruct((total, packed), jnp.bfloat16),
        ],
        scratch_shapes=[pltpu.VMEM((HALO, chans), jnp.float32)],
        name="conv_project",
    )(arrived, halo, weight.astype(jnp.float32), bias.astype(jnp.float32)[None, :], x_weight)


def prepare_kernel(
    states, xc_ref, nm_ref, bc_ref, dtw_ref, dtb_ref, rate_ref, st, dr, end_ref, sum_ref
):
    rows, chans = xc_ref.shape
    group = chans // 128

    @pl.when(pl.program_id(1) == 0)
    def _():
        end_ref[...] = jnp.zeros_like(end_ref)
        sum_ref[...] = jnp.zeros_like(sum_ref)

    raw = jnp.dot(nm_ref[...], dtw_ref[...], preferred_element_type=jnp.float32) + dtb_ref[...]
    step = jnp.maximum(raw, 0.0) + jnp.log1p(jnp.exp(-jnp.abs(raw)))
    drive = step * xc_ref[...].astype(jnp.float32)
    for j in range(group):
        st[pl.ds(j, rows, stride=group), :] = step[:, j * 128 : (j + 1) * 128]
        dr[pl.ds(j, rows, stride=group), :] = drive[:, j * 128 : (j + 1) * 128]

    rates = [rate_ref[n * group : (n + 1) * group, :] for n in range(states)]

    def advance(t, carry):
        at = pl.ds(pl.multiple_of(t * group, group), group)
        s = st[at, :]
        d = dr[at, :]
        base = t * (2 * states)
        after = [
            jnp.exp2(s * rates[n]) * carry[n] + bc_ref[0, 0, base + n] * d for n in range(states)
        ]
        return tuple(after) + (carry[states] + s,)

    carry = tuple(end_ref[0, n * group : (n + 1) * group, :] for n in range(states))
    carry = lax.fori_loop(0, rows, advance, carry + (sum_ref[0],), unroll=4)
    for n in range(states):
        end_ref[0, n * group : (n + 1) * group, :] = carry[n]
    sum_ref[0] = carry[states]


def prepare(xc, normed, bc, dt_weight, dt_bias, rate2, first, parts, steps, block):
    chans = xc.shape[1]
    states2 = bc.shape[2] // block
    states = states2 // 2
    group = chans // 128
    rank = normed.shape[1]
    whole = lambda p, i: (0, 0)
    tile = lambda p, i: ((first + p) * steps + i, 0)
    mine = lambda p, i: (p * steps + i, 0)
    total = parts * steps * block
    return pl.pallas_call(
        functools.partial(prepare_kernel, states),
        grid=(parts, steps),
        in_specs=[
            pl.BlockSpec((block, chans), tile),
            pl.BlockSpec((block, rank), tile),
            pl.BlockSpec(
                (1, 1, block * states2),
                lambda p, i: ((first + p) * steps + i, 0, 0),
                memory_space=pltpu.SMEM,
            ),
            pl.BlockSpec((rank, chans), whole),
            pl.BlockSpec((1, chans), whole),
            pl.BlockSpec((states * group, 128), whole),
        ],
        out_specs=[
            pl.BlockSpec((block * group, 128), mine),
            pl.BlockSpec((block * group, 128), mine),
            pl.BlockSpec((1, states * group, 128), lambda p, i: (p, 0, 0)),
            pl.BlockSpec((1, group, 128), lambda p, i: (p, 0, 0)),
        ],
        out_shape=[
            jax.ShapeDtypeStruct((total * group, 128), jnp.float32),
            jax.ShapeDtypeStruct((total * group, 128), jnp.float32),
            jax.ShapeDtypeStruct((parts, states * group, 128), jnp.float32),
            jax.ShapeDtypeStruct((parts, group, 128), jnp.float32),
        ],
        cost_estimate=pl.CostEstimate(
            flops=total * chans * (2 * rank + 5 * states),
            bytes_accessed=total * chans * 10,
            transcendentals=total * chans * states,
        ),
        name="prepare",
    )(xc, normed, bc, dt_weight, dt_bias, rate2)


def scan_kernel(
    states, parts, peers, xc_ref, st, dr, bc_ref, rate_ref, skip_ref, h0_ref, out_ref,
    ybuf, ys, hs, send_sem, recv_sem, own_sem,
):
    total, chans = xc_ref.shape
    group = chans // 128
    rows = total // peers
    steps = total // parts // rows
    xs = lax.axis_size("x")
    cores = parts // xs
    x = lax.axis_index("x")
    me = greet(peers)
    columns = out_ref.at[:, pl.ds(pl.multiple_of(me * chans, chans), chans)]
    rates = [rate_ref[n * group : (n + 1) * group, :] for n in range(states)]

    def send(block):
        away = lax.rem(block - me + peers, peers)
        return pltpu.make_async_remote_copy(
            src_ref=ybuf.at[block],
            dst_ref=columns,
            send_sem=send_sem.at[away],
            recv_sem=recv_sem.at[away],
            device_id=device(block),
            device_id_type=MESH,
        )

    own = pltpu.make_async_copy(ybuf.at[me], columns, own_sem)

    def one_block(place_in_order, _):
        turn, i = place_in_order // steps, lax.rem(place_in_order, steps)
        part = lax.rem(turn, cores) * xs + lax.rem(x + 1 + turn // cores, xs)
        block = part * steps + i
        base_row = pl.multiple_of(block * rows, rows)

        @pl.when(i == 0)
        def _():
            hs[...] = h0_ref[part].astype(jnp.float32)

        def advance(t, hidden):
            at = pl.ds(pl.multiple_of((base_row + t) * group, group), group)
            s = st[at, :]
            d = dr[at, :]
            base = (base_row + t) * (2 * states)
            after = []
            sums = [None, None]
            for n in range(states):
                h = jnp.exp2(s * rates[n]) * hidden[n] + bc_ref[base + n] * d
                after.append(h)
                term = bc_ref[base + states + n] * h
                sums[n % 2] = term if sums[n % 2] is None else sums[n % 2] + term
            ys[pl.ds(pl.multiple_of(t * group, group), group), :] = sums[0] + sums[1]
            return tuple(after)

        hidden = tuple(hs[n * group : (n + 1) * group, :] for n in range(states))
        hidden = lax.fori_loop(0, rows, advance, hidden, unroll=4)
        for n in range(states):
            hs[n * group : (n + 1) * group, :] = hidden[n]
        for j in range(group):
            sl = slice(j * 128, (j + 1) * 128)
            skipped = skip_ref[:, sl] * xc_ref[pl.ds(base_row, rows), sl].astype(jnp.float32)
            y = ys[pl.ds(j, rows, stride=group), :] + skipped
            ybuf[block, :, sl] = y.astype(jnp.bfloat16)

        @pl.when(block == me)
        def _():
            own.start()

        @pl.when(block != me)
        def _():
            send(block).start()

        return 0

    lax.fori_loop(0, peers, one_block, 0)
    own.wait()
    for k in range(1, peers):
        send(lax.rem(me + k, peers)).wait()


def scan(xc, st, dr, bc, rate2, skip, start, parts, peers):
    total, chans = xc.shape
    states = bc.shape[0] // total // 2
    group = chans // 128
    rows = total // peers
    vmem = pl.BlockSpec(memory_space=pltpu.VMEM)
    return pl.pallas_call(
        functools.partial(scan_kernel, states, parts, peers),
        in_specs=[vmem, vmem, vmem, pl.BlockSpec(memory_space=pltpu.SMEM), vmem, vmem, vmem],
        out_specs=pl.BlockSpec(memory_space=pl.ANY),
        out_shape=jax.ShapeDtypeStruct((rows, peers * chans), jnp.bfloat16),
        scratch_shapes=[
            pltpu.VMEM((peers, rows, chans), jnp.bfloat16),
            pltpu.VMEM((rows * group, 128), jnp.float32),
            pltpu.VMEM((states * group, 128), jnp.float32),
            pltpu.SemaphoreType.DMA((peers,)),
            pltpu.SemaphoreType.DMA((peers,)),
            pltpu.SemaphoreType.DMA,
        ],
        compiler_params=pltpu.CompilerParams(collective_id=1, has_side_effects=True),
        name="selective_scan",
    )(xc, st, dr, bc, rate2, skip, start)


PLANE = ("core", "x", "y")


def local(
    sizes,
    conv_input,
    gate_input,
    conv_weight,
    conv_bias,
    x_weight,
    dt_gain,
    dt_weight,
    dt_bias,
    a_log,
    skip,
):
    depth, parts = sizes
    rank, chans = dt_weight.shape
    states = a_log.shape[0]
    rows = conv_input.shape[0]
    group = chans // 128
    cores = parts // lax.axis_size("x")
    place = lambda z, b: z * parts + b % (parts // cores) * cores + b // (parts // cores)
    swap = [(place(a, b), place(b, a)) for a in range(depth) for b in range(parts)]
    move = lambda v: lax.ppermute(v, ("z", "x", "core"), swap)
    following = [(z, z + 1) for z in range(depth - 1)]
    onward = lambda v: lax.ppermute(v, "z", following)

    conv_pack = move(jnp.concatenate([conv_weight, conv_bias[None, :]], 0))
    x_weight = move(x_weight)
    dt_weight = move(dt_weight)
    scan_pack = move(jnp.concatenate([a_log, dt_bias[None, :], skip[None, :]], 0))
    width = conv_weight.shape[0]
    conv_weight, conv_bias = conv_pack[:width], conv_pack[width]

    arrived = exchange(conv_input, conv_input.shape[1] // chans)
    span = arrived.shape[0] // parts
    halo = onward(arrived.reshape(parts, span, chans)[:, span - HALO :]).astype(jnp.float32)
    conv_out, partial_value = conv_project(
        arrived, halo, conv_weight, conv_bias, x_weight, parts, rows, rank
    )
    everyone = reduce_norm(partial_value, dt_gain, arrived.shape[0] // rows, rank, 2 * states)
    normed_all = everyone[:, :rank]
    bc_all = everyone[:, rank : rank + 2 * states].astype(jnp.float32) + everyone[
        :, rank + 2 * states : rank + 4 * states
    ].astype(jnp.float32)
    bc_all = bc_all.reshape(-1, 1, rows * 2 * states)
    rate2 = (-jnp.exp(scan_pack[:states]) * LOG2E).reshape(states * group, 128)
    dt_bias, skip = scan_pack[states : states + 1], scan_pack[states + 1 :]
    steps = span // rows
    st, dr, ends, sums = prepare(
        conv_out, normed_all, bc_all, dt_weight, dt_bias, rate2, 0, parts, steps, rows
    )
    decay = jnp.exp2(sums[:, None] * rate2.reshape(1, states, group, 128)).reshape(ends.shape)
    start = onward(ends.astype(jnp.bfloat16))
    for _ in range(depth - 2):
        start = onward((decay * start.astype(jnp.float32) + ends).astype(jnp.bfloat16))
    returned = scan(
        conv_out, st, dr, bc_all.reshape(-1), rate2, skip, start, parts, arrived.shape[0] // rows
    )
    return (returned.astype(jnp.float32) * jax.nn.silu(gate_input.astype(jnp.float32))).astype(
        jnp.bfloat16
    )


def solution(mesh):
    seq, batch = mesh.shape["seq"], mesh.shape["batch"]
    cores = 2
    grid = Mesh(
        mesh.devices.reshape(batch, seq // batch, batch // cores, cores), ("z", "y", "x", "core")
    )
    seqs = ("z", "y")
    rows = P(("x", "core", "z", "y"), None)
    return jax.shard_map(
        functools.partial(local, (batch, batch)),
        mesh=grid,
        in_specs=(
            rows,
            rows,
            P(None, seqs),
            P(seqs),
            P(seqs, None),
            P(),
            P(None, seqs),
            P(seqs),
            P(None, seqs),
            P(seqs),
        ),
        out_specs=rows,
        check_vma=False,
    )
```
